32 devices in a mesh: dp: 1, tp: 32 (over x, y, z, core).
Axes of the slice: x: 2, y: 2, z: 4, core: 2. Of those that a mesh axis runs over, the one named last changes fastest.
Arguments:
- x: bfloat16 [2048, 7168], P('dp')
- w_gate: bfloat16 [7168, 20480], P(None, 'tp')
- w_up: bfloat16 [7168, 20480], P(None, 'tp')
- w_down: bfloat16 [20480, 7168], P('tp')
Outputs:
- output: bfloat16 [2048, 7168], P('dp')
All inputs are finite; a program needn't handle non-finite values.
Results may differ from the reference program's by a relative error of at most 0.016.
Values are sent between devices in bfloat16 or wider.
A program may use at most 2 GiB of HBM per device.

```python
import jax
import jax.numpy as jnp

ROWS = 2048
D = 7168
FF = 20480


def setup_inputs(seed: int = 0, part: int = 0) -> dict:
    kx, kg, ku, kd = jax.random.split(jax.random.key(seed), 4)
    drawn = {
        "x": jax.random.normal(jax.random.fold_in(kx, part), (ROWS, D), jnp.float32),
        "w_gate": jax.random.normal(kg, (D, FF), jnp.float32) * D**-0.5,
        "w_up": jax.random.normal(ku, (D, FF), jnp.float32) * D**-0.5,
        "w_down": jax.random.normal(kd, (FF, D), jnp.float32) * FF**-0.5,
    }
    return {k: v.astype(jnp.bfloat16) for k, v in drawn.items()}


def reference(x, w_gate, w_up, w_down):
    gate = jnp.dot(x, w_gate, preferred_element_type=jnp.float32)
    up = jnp.dot(x, w_up, preferred_element_type=jnp.float32)
    hidden = (jax.nn.silu(gate) * up).astype(jnp.bfloat16)
    return jnp.dot(hidden, w_down, preferred_element_type=jnp.float32).astype(jnp.bfloat16)
```

```python
import functools

import jax
import jax.numpy as jnp
from jax import lax
from jax.experimental import pallas as pl
from jax.experimental.pallas import tpu as pltpu
from jax.sharding import PartitionSpec as P

MESH = pl.DeviceIdType.MESH
F32, BF16 = jnp.float32, jnp.bfloat16

ROWS_PER_CHUNK = 128
K_BLOCKS = 4
OFF = (0, 1, 2, 3, 4, 5, 6, 7, 8, 9, 10, 11)
KP = 2 * (OFF[1] - OFF[0])
KX = 2 * (OFF[2] - OFF[1])
KZ1 = 2 * OFF[5] - OFF[2] - OFF[4]
KZ2 = OFF[5] + OFF[4] - 2 * OFF[3]
KZ3 = OFF[5] - OFF[2]
KY = 2 * (OFF[6] - OFF[5])
KT = OFF[1] - OFF[0]
KA = OFF[5] - OFF[1]
KYS = max(2, OFF[6] - OFF[5] + 1)
M1 = 2 * (OFF[7] - OFF[6])
M2 = max(2 * (OFF[8] - OFF[7]), OFF[8] - OFF[6])
M3 = OFF[9] - OFF[6]
MX = 2 * (OFF[10] - OFF[9])
MP = 2 * (OFF[11] - OFF[10])
SEND = 2
GSEND = 4


def kernel(R, x_ref, wg_ref, wu_ref, wd_ref, y_ref, wgu, wdv, xbuf, term, acc, pairsend, pairrecv,
           xsend, xrecv, z1send, z1recv, z2send, z2recv, z3send, z3recv, ysend, yrecv, fin,
           w_sem, x_sem, sp, rp, sx, rx, sz1, rz1, sz2, rz2, sz3, rz3, sy, ry, sl,
           sa1, ra1, sa2, ra2, sa3, ra3, sxa, rxa, spa, rpa):
    N = x_ref.shape[0] // R
    D = x_ref.shape[1]
    F = wg_ref.shape[1]
    W = D // 8
    Q = R // 4
    KB = D // K_BLOCKS

    me = lax.axis_index("tp")
    c = lax.rem(me, 2)
    z = lax.rem(me // 2, 4)
    yy = lax.rem(me // 8, 2)
    xx = me // 16
    odd = lax.rem(z, 2)
    s = z // 2
    is_end = lax.rem(z, 3) == 0
    is_mid = lax.rem(z, 3) != 0
    pair = me + 1 - 2 * c
    xp = me + 16 - 32 * xx
    yp = me + 8 - 16 * yy
    side = me + 2 - 4 * odd
    mid = jnp.where(is_mid, me + 6 - 4 * z, me)
    first = (xp, yp)
    last = (yp, xp)
    f = (xx, yy)

    def quarter(j):
        return pl.multiple_of((j + s * (3 - 2 * j)) * Q, Q)

    def remote(src, dst, ss, rs, dev):
        return pltpu.make_async_remote_copy(
            src_ref=src, dst_ref=dst, send_sem=ss, recv_sem=rs, device_id={"tp": dev}, device_id_type=MESH
        )

    def weight_copies(b):
        rows = pl.ds(b * KB, KB)
        return (
            pltpu.make_async_copy(wg_ref.at[rows], wgu.at[rows, pl.ds(0, F)], w_sem.at[b, 0]),
            pltpu.make_async_copy(wu_ref.at[rows], wgu.at[rows, pl.ds(F, F)], w_sem.at[b, 1]),
        )

    down_copy = pltpu.make_async_copy(wd_ref, wdv, w_sem.at[K_BLOCKS, 0])

    def x_copy(k):
        rows = pl.ds(pl.multiple_of(k * R, R), R)
        return pltpu.make_async_copy(x_ref.at[rows], xbuf.at[lax.rem(k, 2)], x_sem.at[lax.rem(k, 2)])

    x_copy(0).start()
    for b in range(K_BLOCKS):
        for copy in weight_copies(b):
            copy.start()
    down_copy.start()

    barrier = pltpu.get_barrier_semaphore()
    for dev in (pair, xp, yp, side):
        pl.semaphore_signal(barrier, inc=1, device_id={"tp": dev}, device_id_type=MESH)

    @pl.when(is_mid)
    def _():
        pl.semaphore_signal(barrier, inc=1, device_id={"tp": mid}, device_id_type=MESH)
        pl.semaphore_wait(barrier, 5)

    @pl.when(is_end)
    def _():
        pl.semaphore_wait(barrier, 4)

    def c_pair(k):
        a, b = lax.rem(k, SEND), lax.rem(k, KP)
        return remote(pairsend.at[a], pairrecv.at[b], sp.at[a], rp.at[b], pair)

    def c_first(k, t):
        a, b = lax.rem(k, SEND), lax.rem(k, KX)
        return remote(xsend.at[a, t], xrecv.at[b, t], sx.at[t, a], rx.at[t, b], first[t])

    def c_z1(k):
        a, b = lax.rem(k, SEND), lax.rem(k, KZ1)
        return remote(z1send.at[a], z1recv.at[b], sz1.at[a], rz1.at[b], side)

    def c_z2(k):
        a, b = lax.rem(k, SEND), lax.rem(k, KZ2)
        return remote(z2send.at[a], z2recv.at[b], sz2.at[a], rz2.at[b], mid)

    def c_z3(k):
        a, b = lax.rem(k, SEND), lax.rem(k, KZ3)
        return remote(z3send.at[a], z3recv.at[b], sz3.at[a], rz3.at[b], side)

    def c_last(k, t):
        a, b = lax.rem(k, KYS), lax.rem(k, KY)
        return remote(ysend.at[a, t], yrecv.at[b, t], sy.at[t, a], ry.at[t, b], last[t])

    def block(t, flip=False):
        h = 1 - f[t] if flip else f[t]
        return pl.ds(pl.multiple_of((c * 4 + t * 2 + h) * W, 128), W)

    def y_quarter(k, j, t):
        return y_ref.at[pl.ds(pl.multiple_of(k * R + quarter(j), Q), Q), block(t)]

    def y_own(k, t):
        return y_ref.at[pl.ds(pl.multiple_of(k * R + z * Q, Q), Q), block(t)]

    def c_local(k, t):
        a = lax.rem(k, SEND)
        return pltpu.make_async_copy(fin.at[a, t], y_own(k, t), sl.at[t, a])

    def c_a1(k, t, way):
        a, b = lax.rem(k, SEND), lax.rem(k, M1)
        return remote(fin.at[a, t], y_own(k, t), sa1.at[way, t, a], ra1.at[way, t, b], (side, mid)[way])

    def c_a2(k, t, way):
        a, b = lax.rem(k, GSEND), lax.rem(k, M2)
        piece = y_quarter(k, (2, 0)[way], t)
        return remote(piece, piece, sa2.at[way, t, a], ra2.at[t, b], (side, mid)[way])

    def c_a3(k, t):
        a, b = lax.rem(k, GSEND), lax.rem(k, M3)
        piece = y_quarter(k, 3, t)
        return remote(piece, piece, sa3.at[t, a], ra3.at[t, b], side)

    def c_xa(k, t):
        a, b = lax.rem(k, GSEND), lax.rem(k, MX)
        piece = y_ref.at[pl.ds(pl.multiple_of(k * R, R), R), block(t)]
        return remote(piece, piece, sxa.at[t, a], rxa.at[t, b], first[t])

    def c_pa(k):
        a, b = lax.rem(k, GSEND), lax.rem(k, MP)
        piece = y_ref.at[pl.ds(pl.multiple_of(k * R, R), R), pl.ds(pl.multiple_of(c * 4 * W, 128), 4 * W)]
        return remote(piece, piece, spa.at[a], rpa.at[b], pair)

    def s0(k):
        @pl.when(k + 1 < N)
        def _():
            x_copy(k + 1).start()

        x_copy(k).wait()
        xs = lax.rem(k, 2)
        h = None
        for b in range(K_BLOCKS):
            @pl.when(k == 0)
            def _():
                for copy in weight_copies(b):
                    copy.wait()

            part = jnp.dot(xbuf[xs, :, b * KB:(b + 1) * KB], wgu[b * KB:(b + 1) * KB, :], preferred_element_type=F32)
            h = part if h is None else h + part
        hidden = (jax.nn.silu(h[:, :F]) * h[:, F:]).astype(BF16)

        @pl.when(k == 0)
        def _():
            down_copy.wait()

        for t in range(2):
            cols = pl.ds(pl.multiple_of((1 - c) * 4 * W + t * 2 * W, 128), 2 * W)
            part = jnp.dot(hidden, wdv[:, cols], preferred_element_type=F32)
            for i in range(2):
                pairsend[lax.rem(k, SEND), t, i] = part[:, i * W:(i + 1) * W].astype(BF16)
        c_pair(k).start()
        for t in range(2):
            cols = pl.ds(pl.multiple_of(c * 4 * W + t * 2 * W, 128), 2 * W)
            part = jnp.dot(hidden, wdv[:, cols], preferred_element_type=F32)
            for i in range(2):
                term[lax.rem(k, KT), t, i] = part[:, i * W:(i + 1) * W]

    def s1(k):
        c_pair(k).wait_recv()
        a, b, kt, ka = lax.rem(k, SEND), lax.rem(k, KP), lax.rem(k, KT), lax.rem(k, KA)
        for t in range(2):
            h = 1 - f[t]
            xsend[a, t] = (term[kt, t, h] + pairrecv[b, t, h].astype(F32)).astype(BF16)
            c_first(k, t).start()
        for t in range(2):
            h = f[t]
            acc[ka, t] = term[kt, t, h] + pairrecv[b, t, h].astype(F32)

    def s2(k):
        a, b, ka = lax.rem(k, SEND), lax.rem(k, KX), lax.rem(k, KA)
        for t in range(2):
            c_first(k, t).wait_recv()
            acc[ka, t] = acc[ka, t] + xrecv[b, t].astype(F32)

        @pl.when(is_end)
        def _():
            for j in range(1, 4):
                for t in range(2):
                    z1send[a, j - 1, t] = acc[ka, t, pl.ds(quarter(j), Q)].astype(BF16)
            c_z1(k).start()

    def s3(k):
        @pl.when(is_mid)
        def _():
            c_z1(k).wait_recv()
            a, b, ka = lax.rem(k, SEND), lax.rem(k, KZ1), lax.rem(k, KA)
            for j in range(2, 4):
                for t in range(2):
                    z2send[a, j - 2, t] = (
                        acc[ka, t, pl.ds(quarter(j), Q)] + z1recv[b, j - 1, t].astype(F32)
                    ).astype(BF16)
            c_z2(k).start()

    def s4(k):
        @pl.when(is_mid)
        def _():
            c_z2(k).wait_recv()
            a, b, ka = lax.rem(k, SEND), lax.rem(k, KZ2), lax.rem(k, KA)
            for t in range(2):
                z3send[a, t] = (acc[ka, t, pl.ds(quarter(0), Q)] + z2recv[b, 1, t].astype(F32)).astype(BF16)
            c_z3(k).start()

    def s5(k):
        a, ka = lax.rem(k, KYS), lax.rem(k, KA)

        @pl.when(is_mid)
        def _():
            b1, b2 = lax.rem(k, KZ1), lax.rem(k, KZ2)
            for t in range(2):
                ysend[a, t] = (
                    acc[ka, t, pl.ds(quarter(1), Q)] + z1recv[b1, 0, t].astype(F32) + z2recv[b2, 0, t].astype(F32)
                ).astype(BF16)

        @pl.when(is_end)
        def _():
            c_z3(k).wait_recv()
            b3 = lax.rem(k, KZ3)
            for t in range(2):
                ysend[a, t] = (acc[ka, t, pl.ds(quarter(0), Q)] + z3recv[b3, t].astype(F32)).astype(BF16)

        for t in range(2):
            c_last(k, t).start()

    def s6(k):
        a, b, g = lax.rem(k, KYS), lax.rem(k, KY), lax.rem(k, SEND)
        for t in range(2):
            c_last(k, t).wait_recv()
            fin[g, t] = (ysend[a, t].astype(F32) + yrecv[b, t].astype(F32)).astype(BF16)
        for t in range(2):
            c_local(k, t).start()
            c_a1(k, t, 0).start()

        @pl.when(is_mid)
        def _():
            for t in range(2):
                c_a1(k, t, 1).start()

    def s7(k):
        for t in range(2):
            c_a1(k, t, 0).wait_recv()

        @pl.when(is_mid)
        def _():
            for t in range(2):
                c_a2(k, t, 1).start()
            for t in range(2):
                c_a1(k, t, 1).wait_recv()
                c_a2(k, t, 0).start()

    def s8(k):
        for t in range(2):
            c_a2(k, t, 0).wait_recv()

        @pl.when(is_mid)
        def _():
            for t in range(2):
                c_a3(k, t).start()

    def s9(k):
        @pl.when(is_end)
        def _():
            for t in range(2):
                c_a3(k, t).wait_recv()

        for t in range(2):
            c_xa(k, t).start()

    def s10(k):
        for t in range(2):
            c_xa(k, t).wait_recv()
        c_pa(k).start()

    def s11(k):
        c_pa(k).wait_recv()

    def d0(k):
        c_pair(k).wait_send()

    def d1(k):
        for t in range(2):
            c_first(k, t).wait_send()

    def d2(k):
        @pl.when(is_end)
        def _():
            c_z1(k).wait_send()

    def d3(k):
        @pl.when(is_mid)
        def _():
            c_z2(k).wait_send()

    def d4(k):
        @pl.when(is_mid)
        def _():
            c_z3(k).wait_send()

    def d5(k):
        for t in range(2):
            c_last(k, t).wait_send()

    def d6(k):
        for t in range(2):
            c_local(k, t).wait()
            c_a1(k, t, 0).wait_send()

        @pl.when(is_mid)
        def _():
            for t in range(2):
                c_a1(k, t, 1).wait_send()

    def d7(k):
        @pl.when(is_mid)
        def _():
            for t in range(2):
                c_a2(k, t, 1).wait_send()
                c_a2(k, t, 0).wait_send()

    def d8(k):
        @pl.when(is_mid)
        def _():
            for t in range(2):
                c_a3(k, t).wait_send()

    def d9(k):
        for t in range(2):
            c_xa(k, t).wait_send()

    def d10(k):
        c_pa(k).wait_send()

    stages = (
        (s0, d0, SEND), (s1, d1, SEND), (s2, d2, SEND), (s3, d3, SEND), (s4, d4, SEND), (s5, d5, KYS),
        (s6, d6, SEND), (s7, d7, GSEND), (s8, d8, GSEND), (s9, d9, GSEND), (s10, d10, GSEND), (s11, None, 0),
    )
    ticks = N + max(off + lag for off, (_, _, lag) in zip(OFF, stages))

    def tick(i, carry):
        for off, (run, drain, lag) in reversed(tuple(zip(OFF, stages))):
            if drain is not None:
                k_old = i - off - lag

                @pl.when((k_old >= 0) & (k_old < N))
                def _():
                    drain(k_old)

            k = i - off

            @pl.when((k >= 0) & (k < N))
            def _():
                run(k)

        return carry

    lax.fori_loop(0, ticks, tick, 0)


def solution(mesh):
    def step(x, w_gate, w_up, w_down):
        rows, D = x.shape
        F = w_gate.shape[1]
        R = min(ROWS_PER_CHUNK, rows // 8)
        W, Q = D // 8, R // 4
        any_spec = pl.BlockSpec(memory_space=pl.ANY)
        dma = lambda *shape: pltpu.SemaphoreType.DMA(shape)
        return pl.pallas_call(
            functools.partial(kernel, R),
            out_shape=jax.ShapeDtypeStruct((rows, D), BF16),
            in_specs=[any_spec] * 4,
            out_specs=any_spec,
            scratch_shapes=[
                pltpu.VMEM((D, 2 * F), BF16),
                pltpu.VMEM((F, D), BF16),
                pltpu.VMEM((2, R, D), BF16),
                pltpu.VMEM((KT, 2, 2, R, W), F32),
                pltpu.VMEM((KA, 2, R, W), F32),
                pltpu.VMEM((SEND, 2, 2, R, W), BF16),
                pltpu.VMEM((KP, 2, 2, R, W), BF16),
                pltpu.VMEM((SEND, 2, R, W), BF16),
                pltpu.VMEM((KX, 2, R, W), BF16),
                pltpu.VMEM((SEND, 3, 2, Q, W), BF16),
                pltpu.VMEM((KZ1, 3, 2, Q, W), BF16),
                pltpu.VMEM((SEND, 2, 2, Q, W), BF16),
                pltpu.VMEM((KZ2, 2, 2, Q, W), BF16),
                pltpu.VMEM((SEND, 2, Q, W), BF16),
                pltpu.VMEM((KZ3, 2, Q, W), BF16),
                pltpu.VMEM((KYS, 2, Q, W), BF16),
                pltpu.VMEM((KY, 2, Q, W), BF16),
                pltpu.VMEM((SEND, 2, Q, W), BF16),
                dma(K_BLOCKS + 1, 2), dma(2),
                dma(SEND), dma(KP),
                dma(2, SEND), dma(2, KX),
                dma(SEND), dma(KZ1),
                dma(SEND), dma(KZ2),
                dma(SEND), dma(KZ3),
                dma(2, KYS), dma(2, KY),
                dma(2, SEND),
                dma(2, 2, SEND), dma(2, 2, M1),
                dma(2, 2, GSEND), dma(2, M2),
                dma(2, GSEND), dma(2, M3),
                dma(2, GSEND), dma(2, MX),
                dma(GSEND), dma(MP),
            ],
            compiler_params=pltpu.CompilerParams(
                collective_id=0, has_side_effects=True, vmem_limit_bytes=67043328
            ),
            name="mlp_all_reduce",
        )(x, w_gate, w_up, w_down)

    return jax.shard_map(
        step,
        mesh=mesh,
        in_specs=(P("dp", None), P(None, "tp"), P(None, "tp"), P("tp", None)),
        out_specs=P("dp", None),
        check_vma=False,
    )
```

```python
import functools

import jax
import jax.numpy as jnp
from jax import lax
from jax.experimental import pallas as pl
from jax.experimental.pallas import tpu as pltpu
from jax.sharding import PartitionSpec as P

MESH = pl.DeviceIdType.MESH
F32, BF16 = jnp.float32, jnp.bfloat16

ROWS_PER_CHUNK = 128
PIECES = 2
TAIL = 2
OFF = (0, 1, 3, 4, 5, 6, 7)
GOFF = (0, 2, 4, 6, 8, 10)
KP = 2 * (OFF[1] - OFF[0])
KX = 2 * (OFF[2] - OFF[1])
KZ1 = OFF[5] - OFF[2]
KZ2 = 2 * (OFF[4] - OFF[3])
KZ3 = OFF[5] - OFF[2]
KY = 2 * (OFF[6] - OFF[5])
KT = OFF[1] - OFF[0]
KO = OFF[5] - OFF[1]
KI = OFF[3] - OFF[1]
SEND = 3
PSEND = 2
KC1 = OFF[4] - OFF[1]
KC2 = 2 * (OFF[3] - OFF[2])
KC3 = OFF[5] - OFF[1]
KC4 = 2 * (OFF[5] - OFF[4])
KYS = max(SEND, OFF[6] - OFF[5] + 1)
M1 = GOFF[3] - GOFF[0]
M2 = 2 * (GOFF[2] - GOFF[1])
M3 = GOFF[3] - GOFF[0]
MO = 2 * GOFF[4] - GOFF[0] - GOFF[2]
MI = 2 * (GOFF[4] - GOFF[2])
MP = 2 * (GOFF[5] - GOFF[4])
GSEND = 6


def split(W):
    return W * 5 // 7 // 128 * 128 if W > 256 else W // 2


def kernel(R, x_ref, wg_ref, wu_ref, wd_ref, y_ref, xbuf, hidden, term, acco, acci, pairsend, pairrecv,
           xsend, xrecv, z1send, z1recv, z2send, z2recv, z3send, z3recv, ysend, yrecv, fin,
           accco, accci, c1send, c1recv, c2send, c2recv, c3send, c3recv, c4send, c4recv,
           w_sem, x_sem, sp, rp, sx, rx, sz1, rz1, sz2, rz2, sz3, rz3, sy, ry,
           sc1, rc1, sc2, rc2, sc3, rc3, sc4, rc4, ready,
           sa1, ra1, sa2, ra2, sa3, ra3, sxo, rxo, sxi, rxi, spa, rpa):
    N = x_ref.shape[0] // R
    D = x_ref.shape[1]
    F = wg_ref.shape[1]
    W = D // 8
    W1 = split(W)
    Q = R // 2
    G = Q // PIECES
    NG = N * PIECES
    KB = y_ref.shape[0] - F
    NB = D // KB
    REST = D - NB * KB
    assert 2 * REST <= KB and NB * 2 * F + F <= D

    me = lax.axis_index("tp")
    c = lax.rem(me, 2)
    z = lax.rem(me // 2, 4)
    yy = lax.rem(me // 8, 2)
    xx = me // 16
    odd = lax.rem(z, 2)
    s = z // 2
    is_end = lax.rem(z, 3) == 0
    is_mid = lax.rem(z, 3) != 0
    pair = me + 1 - 2 * c
    xp = me + 16 - 32 * xx
    yp = me + 8 - 16 * yy
    side = me + 2 - 4 * odd
    mid = jnp.where(is_mid, me + 6 - 4 * z, me)
    first = (xp, yp)
    last = (yp, xp)
    f = (xx, yy)

    out_rows = pl.multiple_of((1 - s) * Q, Q)
    in_rows = pl.multiple_of(s * Q, Q)

    def remote(src, dst, ss, rs, dev):
        return pltpu.make_async_remote_copy(
            src_ref=src, dst_ref=dst, send_sem=ss, recv_sem=rs, device_id={"tp": dev}, device_id_type=MESH
        )

    def weight_copies(b):
        copies = []
        for i, ref in enumerate((wg_ref, wu_ref)):
            if b < NB:
                dst = y_ref.at[pl.ds(F, KB), pl.ds((2 * b + i) * F, F)]
                src = ref.at[pl.ds(b * KB, KB)]
            else:
                dst = y_ref.at[pl.ds(F + i * REST, REST), pl.ds(NB * 2 * F, F)]
                src = ref.at[pl.ds(NB * KB, REST)]
            copies.append(pltpu.make_async_copy(src, dst, w_sem.at[b, i]))
        return copies

    down_copy = pltpu.make_async_copy(wd_ref, y_ref.at[pl.ds(0, F)], w_sem.at[NB + 1, 0])

    def x_copy(k):
        rows = pl.ds(pl.multiple_of(k * R, R), R)
        return pltpu.make_async_copy(x_ref.at[rows], xbuf.at[lax.rem(k, 2)], x_sem.at[lax.rem(k, 2)])

    x_copy(0).start()
    for b in range(NB + 1):
        for copy in weight_copies(b):
            copy.start()
    down_copy.start()

    barrier = pltpu.get_barrier_semaphore()
    for dev in (pair, xp, yp, side):
        pl.semaphore_signal(barrier, inc=1, device_id={"tp": dev}, device_id_type=MESH)

    @pl.when(is_mid)
    def _():
        pl.semaphore_signal(barrier, inc=1, device_id={"tp": mid}, device_id_type=MESH)
        pl.semaphore_wait(barrier, 5)

    @pl.when(is_end)
    def _():
        pl.semaphore_wait(barrier, 4)

    def c_pair(k):
        a, b = lax.rem(k, PSEND), lax.rem(k, KP)
        return remote(pairsend.at[a], pairrecv.at[b], sp.at[a], rp.at[b], pair)

    def c_first(k, t):
        a, b = lax.rem(k, SEND), lax.rem(k, KX)
        return remote(xsend.at[a, t], xrecv.at[b, t], sx.at[t, a], rx.at[t, b], first[t])

    def c_z1(k):
        a, b = lax.rem(k, SEND), lax.rem(k, KZ1)
        return remote(z1send.at[a], z1recv.at[b], sz1.at[a], rz1.at[b], side)

    def c_z2(k):
        a, b = lax.rem(k, SEND), lax.rem(k, KZ2)
        return remote(z2send.at[a], z2recv.at[b], sz2.at[a], rz2.at[b], mid)

    def c_z3(k):
        a, b = lax.rem(k, SEND), lax.rem(k, KZ3)
        return remote(z3send.at[a], z3recv.at[b], sz3.at[a], rz3.at[b], side)

    def c_last(k, t):
        a, b = lax.rem(k, KYS), lax.rem(k, KY)
        return remote(ysend.at[a, t], yrecv.at[b, t], sy.at[t, a], ry.at[t, b], last[t])

    def c_c1(k):
        a, b = lax.rem(k, SEND), lax.rem(k, KC1)
        return remote(c1send.at[a], c1recv.at[b], sc1.at[a], rc1.at[b], side)

    def c_c2(k):
        a, b = lax.rem(k, SEND), lax.rem(k, KC2)
        return remote(c2send.at[a], c2recv.at[b], sc2.at[a], rc2.at[b], mid)

    def c_c3(k):
        a, b = lax.rem(k, SEND), lax.rem(k, KC3)
        return remote(c3send.at[a], c3recv.at[b], sc3.at[a], rc3.at[b], side)

    def c_c4(k, t):
        a, b = lax.rem(k, SEND), lax.rem(k, KC4)
        return remote(c4send.at[a, t], c4recv.at[b, t], sc4.at[t, a], rc4.at[t, b], first[t])

    def block(t, flip=False):
        h = 1 - f[t] if flip else f[t]
        return pl.ds(pl.multiple_of((c * 4 + t * 2 + h) * W, 128), W)

    def y_piece(p, at, t):
        row = (p // PIECES) * R + at + lax.rem(p, PIECES) * G
        return y_ref.at[pl.ds(pl.multiple_of(row, G), G), block(t)]

    def fin_piece(p, t):
        return fin.at[p // PIECES, t, pl.ds(pl.multiple_of(lax.rem(p, PIECES) * G, G), G)]

    def c_a1(p, t):
        a, b = lax.rem(p, GSEND), lax.rem(p, M1)
        return remote(fin_piece(p, t), y_piece(p, out_rows, t), sa1.at[t, a], ra1.at[t, b], side)

    def c_a2(p, t):
        a, b = lax.rem(p, GSEND), lax.rem(p, M2)
        piece = y_piece(p, out_rows, t)
        return remote(piece, piece, sa2.at[t, a], ra2.at[t, b], mid)

    def c_a3(p, t):
        a, b = lax.rem(p, GSEND), lax.rem(p, M3)
        piece = y_piece(p, in_rows, t)
        return remote(piece, piece, sa3.at[t, a], ra3.at[t, b], side)

    def c_xo(p, t, src=None):
        a, b = lax.rem(p, GSEND), lax.rem(p, MO)
        piece = y_piece(p, out_rows, t)
        return remote(piece if src is None else src, piece, sxo.at[t, a], rxo.at[t, b], first[t])

    def c_xi(p, t):
        a, b = lax.rem(p, GSEND), lax.rem(p, MI)
        piece = y_piece(p, in_rows, t)
        return remote(piece, piece, sxi.at[t, a], rxi.at[t, b], first[t])

    def c_pa(p, h):
        a, b = lax.rem(p, GSEND), lax.rem(p, MP)
        row = (p // PIECES) * R + h * Q + lax.rem(p, PIECES) * G
        piece = y_ref.at[pl.ds(pl.multiple_of(row, G), G), pl.ds(pl.multiple_of(c * 4 * W, 128), 4 * W)]
        return remote(piece, piece, spa.at[h, a], rpa.at[h, b], pair)

    def h0(k):
        @pl.when(k + 1 < N)
        def _():
            x_copy(k + 1).start()

        x_copy(k).wait()
        xs = lax.rem(k, 2)
        h = None
        for b in range(NB + 1):
            @pl.when(k == 0)
            def _():
                for copy in weight_copies(b):
                    copy.wait()

            if b < NB:
                part = jnp.dot(
                    xbuf[xs, :, b * KB:(b + 1) * KB],
                    y_ref[F:F + KB, b * 2 * F:(b + 1) * 2 * F],
                    preferred_element_type=F32,
                )
                h = part if h is None else h + part
        gate, up = (
            h[:, i * F:(i + 1) * F] + jnp.dot(
                xbuf[xs, :, NB * KB:],
                y_ref[F + i * REST:F + (i + 1) * REST, NB * 2 * F:NB * 2 * F + F],
                preferred_element_type=F32,
            )
            for i in range(2)
        )
        hidden[...] = (jax.nn.silu(gate) * up).astype(BF16)

    def s0(k):
        @pl.when(k == 0)
        def _():
            down_copy.wait()

        for t in range(2):
            cols = pl.ds(pl.multiple_of((1 - c) * 4 * W + t * 2 * W, 128), 2 * W)
            part = jnp.dot(hidden[...], y_ref[:F, cols], preferred_element_type=F32)
            for i in range(2):
                pairsend[lax.rem(k, PSEND), t, i] = part[:, i * W:(i + 1) * W].astype(BF16)
        c_pair(k).start()
        for t in range(2):
            cols = pl.ds(pl.multiple_of(c * 4 * W + t * 2 * W, 128), 2 * W)
            part = jnp.dot(hidden[...], y_ref[:F, cols], preferred_element_type=F32)
            for i in range(2):
                term[lax.rem(k, KT), t, i] = part[:, i * W:(i + 1) * W]

        @pl.when(k == N - 1)
        def _():
            for dev in (pair, xp, yp, side):
                pl.semaphore_signal(ready, inc=1, device_id={"tp": dev}, device_id_type=MESH)

            @pl.when(is_mid)
            def _():
                pl.semaphore_signal(ready, inc=1, device_id={"tp": mid}, device_id_type=MESH)

    def s1(k):
        c_pair(k).wait_recv()
        a, b, kt = lax.rem(k, SEND), lax.rem(k, KP), lax.rem(k, KT)
        ki, ko = lax.rem(k, KI), lax.rem(k, KO)
        for t in range(2):
            h = 1 - f[t]
            xsend[a, t] = (term[kt, t, h, :, :W1] + pairrecv[b, t, h, :, :W1].astype(F32)).astype(BF16)
            c_first(k, t).start()
        for t in range(2):
            for h in range(2):
                for dst, slot, at in ((accci, ki, in_rows), (accco, ko, out_rows)):
                    rows = pl.ds(at, Q)
                    dst[slot, t, h] = term[kt, t, h, rows, W1:] + pairrecv[b, t, h, rows, W1:].astype(F32)

        @pl.when(is_end)
        def _():
            c1send[a] = accci[ki].astype(BF16)
            c_c1(k).start()

        for t in range(2):
            h = f[t]
            for dst, slot, at in ((acci, ki, in_rows), (acco, ko, out_rows)):
                rows = pl.ds(at, Q)
                dst[slot, t] = term[kt, t, h, rows, :W1] + pairrecv[b, t, h, rows, :W1].astype(F32)

    def s2(k):
        a, b, ki, ko = lax.rem(k, SEND), lax.rem(k, KX), lax.rem(k, KI), lax.rem(k, KO)

        @pl.when(is_mid)
        def _():
            c_c1(k).wait_recv()
            c2send[a] = (accci[ki] + c1recv[lax.rem(k, KC1)].astype(F32)).astype(BF16)
            c_c2(k).start()

        for t in range(2):
            c_first(k, t).wait_recv()
            acci[ki, t] = acci[ki, t] + xrecv[b, t, pl.ds(in_rows, Q)].astype(F32)
            acco[ko, t] = acco[ko, t] + xrecv[b, t, pl.ds(out_rows, Q)].astype(F32)

        @pl.when(is_end)
        def _():
            z1send[a] = acci[ki].astype(BF16)
            c_z1(k).start()

    def s3(k):
        @pl.when(is_mid)
        def _():
            a, b, ki, ko = lax.rem(k, SEND), lax.rem(k, KZ1), lax.rem(k, KI), lax.rem(k, KO)
            c_c2(k).wait_recv()
            c3send[a] = (accco[ko] + c2recv[lax.rem(k, KC2)].astype(F32)).astype(BF16)
            c_c3(k).start()
            c_z1(k).wait_recv()
            z2send[a] = (acci[ki] + z1recv[b].astype(F32)).astype(BF16)
            c_z2(k).start()

    def s4(k):
        a, b, ko = lax.rem(k, SEND), lax.rem(k, KZ2), lax.rem(k, KO)

        @pl.when(is_end)
        def _():
            c_c3(k).wait_recv()
            for t in range(2):
                h = 1 - f[t]
                c4send[a, t] = (accco[ko, t, h] + c3recv[lax.rem(k, KC3), t, h].astype(F32)).astype(BF16)
                c_c4(k, t).start()

        @pl.when(is_mid)
        def _():
            c_z2(k).wait_recv()
            z3send[a] = (acco[ko] + z2recv[b].astype(F32)).astype(BF16)
            c_z3(k).start()

    def s5(k):
        @pl.when(is_end)
        def _():
            a, b, ko = lax.rem(k, KYS), lax.rem(k, KZ3), lax.rem(k, KO)
            for t in range(2):
                h = f[t]
                c_c4(k, t).wait_recv()
                ysend[a, t, :, W1:] = (
                    accco[ko, t, h]
                    + c3recv[lax.rem(k, KC3), t, h].astype(F32)
                    + c4recv[lax.rem(k, KC4), t].astype(F32)
                ).astype(BF16)
            c_z3(k).wait_recv()
            for t in range(2):
                ysend[a, t, :, :W1] = (acco[ko, t] + z3recv[b, t].astype(F32)).astype(BF16)
                c_last(k, t).start()

    def s6(k):
        @pl.when(is_end)
        def _():
            a, b = lax.rem(k, KYS), lax.rem(k, KY)
            for t in range(2):
                c_last(k, t).wait_recv()
                fin[k, t] = (ysend[a, t].astype(F32) + yrecv[b, t].astype(F32)).astype(BF16)

    def open_gather():
        @pl.when(is_mid)
        def _():
            pl.semaphore_wait(ready, 5)

        @pl.when(is_end)
        def _():
            pl.semaphore_wait(ready, 4)

    def g0(p):
        @pl.when(is_end)
        def _():
            for t in range(2):
                c_a1(p, t).start()
                c_xo(p, t, fin_piece(p, t)).start()
            for t in range(2):
                y_piece(p, out_rows, t)[...] = fin_piece(p, t)[...]

    def g1(p):
        @pl.when(is_mid)
        def _():
            for t in range(2):
                c_a1(p, t).wait_recv()
                c_a2(p, t).start()
                c_xo(p, t).start()

    def g2(p):
        @pl.when(is_mid)
        def _():
            for t in range(2):
                c_a2(p, t).wait_recv()
                c_a3(p, t).start()
                c_xi(p, t).start()

    def g3(p):
        @pl.when(is_end)
        def _():
            for t in range(2):
                c_a3(p, t).wait_recv()
                c_xi(p, t).start()

    def g4(p):
        for t in range(2):
            c_xo(p, t).wait_recv()
            c_xi(p, t).wait_recv()
        for h in range(2):
            c_pa(p, h).start()

    def g5(p):
        for h in range(2):
            c_pa(p, h).wait_recv()

    def d0(k):
        c_pair(k).wait_send()

    def d1(k):
        for t in range(2):
            c_first(k, t).wait_send()

        @pl.when(is_end)
        def _():
            c_c1(k).wait_send()

    def d2(k):
        @pl.when(is_end)
        def _():
            c_z1(k).wait_send()

        @pl.when(is_mid)
        def _():
            c_c2(k).wait_send()

    def d3(k):
        @pl.when(is_mid)
        def _():
            c_c3(k).wait_send()
            c_z2(k).wait_send()

    def d4(k):
        @pl.when(is_end)
        def _():
            for t in range(2):
                c_c4(k, t).wait_send()

        @pl.when(is_mid)
        def _():
            c_z3(k).wait_send()

    def d5(k):
        @pl.when(is_end)
        def _():
            for t in range(2):
                c_last(k, t).wait_send()

    def e0(p):
        @pl.when(is_end)
        def _():
            for t in range(2):
                c_a1(p, t).wait_send()
                c_xo(p, t, fin_piece(p, t)).wait_send()

    def e1(p):
        @pl.when(is_mid)
        def _():
            for t in range(2):
                c_a2(p, t).wait_send()
                c_xo(p, t).wait_send()

    def e2(p):
        @pl.when(is_mid)
        def _():
            for t in range(2):
                c_a3(p, t).wait_send()
                c_xi(p, t).wait_send()

    def e3(p):
        @pl.when(is_end)
        def _():
            for t in range(2):
                c_xi(p, t).wait_send()

    def e4(p):
        for h in range(2):
            c_pa(p, h).wait_send()

    reduce_stages = (
        (s0, d0, PSEND), (s1, d1, SEND), (h0, None, 0), (s2, d2, SEND), (s3, d3, SEND), (s4, d4, SEND), (s5, d5, KYS),
        (s6, None, 0),
    )
    gather_stages = (
        (g0, e0, GSEND), (g1, e1, GSEND), (g2, e2, GSEND), (g3, e3, GSEND), (g4, e4, GSEND), (g5, None, 0),
    )

    def advance(i, count, offsets, stages):
        for off, (run, drain, lag) in reversed(tuple(zip(offsets, stages))):
            if drain is not None:
                k_old = i - off - lag

                @pl.when((k_old >= 0) & (k_old < count))
                def _():
                    drain(k_old)

            if run is not None:
                k = i - off

                @pl.when((k >= 0) & (k < count))
                def _():
                    run(k)

    offsets = OFF[:2] + OFF[:1] + OFF[2:]
    tail_stages = ((None, d0, PSEND), reduce_stages[1], (None, None, 0)) + reduce_stages[3:]

    def reduce_tick(i, carry):
        advance(i, N, offsets, reduce_stages)
        return carry

    def gather_tick(u, carry):
        @pl.when(lax.rem(u, TAIL) == 0)
        def _():
            advance(N + u // TAIL, N, offsets, tail_stages)

        advance(u, NG, GOFF, gather_stages)
        return carry

    lax.fori_loop(0, N, reduce_tick, 0)
    open_gather()
    ticks = NG + max(off + lag for off, (_, _, lag) in zip(GOFF, gather_stages))
    lax.fori_loop(0, ticks, gather_tick, 0)


def store_kernel(y_ref, o_ref, sem):
    blocks = sem.shape[0]
    rows = y_ref.shape[0] // blocks
    copies = [
        pltpu.make_async_copy(y_ref.at[pl.ds(i * rows, rows)], o_ref.at[pl.ds(i * rows, rows)], sem.at[i])
        for i in range(blocks)
    ]
    for copy in copies:
        copy.start()
    for copy in copies:
        copy.wait()


def solution(mesh):
    def step(x, w_gate, w_up, w_down):
        rows, D = x.shape
        F = w_gate.shape[1]
        R = min(ROWS_PER_CHUNK, rows // 8)
        W, Q = D // 8, R // 2
        W1 = split(W)
        W3 = W - W1
        any_spec = pl.BlockSpec(memory_space=pl.ANY)
        dma = lambda *shape: pltpu.SemaphoreType.DMA(shape)
        blocks = D // (rows - F) + 2
        y = pl.pallas_call(
            functools.partial(kernel, R),
            out_shape=pltpu.VMEM((rows, D), BF16),
            in_specs=[any_spec] * 4,
            out_specs=pl.BlockSpec(memory_space=pltpu.VMEM),
            scratch_shapes=[
                pltpu.VMEM((2, R, D), BF16),
                pltpu.VMEM((R, F), BF16),
                pltpu.VMEM((KT, 2, 2, R, W), F32),
                pltpu.VMEM((KO, 2, Q, W1), F32),
                pltpu.VMEM((KI, 2, Q, W1), F32),
                pltpu.VMEM((PSEND, 2, 2, R, W), BF16),
                pltpu.VMEM((KP, 2, 2, R, W), BF16),
                pltpu.VMEM((SEND, 2, R, W1), BF16),
                pltpu.VMEM((KX, 2, R, W1), BF16),
                pltpu.VMEM((SEND, 2, Q, W1), BF16),
                pltpu.VMEM((KZ1, 2, Q, W1), BF16),
                pltpu.VMEM((SEND, 2, Q, W1), BF16),
                pltpu.VMEM((KZ2, 2, Q, W1), BF16),
                pltpu.VMEM((SEND, 2, Q, W1), BF16),
                pltpu.VMEM((KZ3, 2, Q, W1), BF16),
                pltpu.VMEM((KYS, 2, Q, W), BF16),
                pltpu.VMEM((KY, 2, Q, W), BF16),
                pltpu.VMEM((rows // R, 2, Q, W), BF16),
                pltpu.VMEM((KO, 2, 2, Q, W3), F32),
                pltpu.VMEM((KI, 2, 2, Q, W3), F32),
                pltpu.VMEM((SEND, 2, 2, Q, W3), BF16),
                pltpu.VMEM((KC1, 2, 2, Q, W3), BF16),
                pltpu.VMEM((SEND, 2, 2, Q, W3), BF16),
                pltpu.VMEM((KC2, 2, 2, Q, W3), BF16),
                pltpu.VMEM((SEND, 2, 2, Q, W3), BF16),
                pltpu.VMEM((KC3, 2, 2, Q, W3), BF16),
                pltpu.VMEM((SEND, 2, Q, W3), BF16),
                pltpu.VMEM((KC4, 2, Q, W3), BF16),
                dma(blocks, 2), dma(2),
                dma(PSEND), dma(KP),
                dma(2, SEND), dma(2, KX),
                dma(SEND), dma(KZ1),
                dma(SEND), dma(KZ2),
                dma(SEND), dma(KZ3),
                dma(2, KYS), dma(2, KY),
                dma(SEND), dma(KC1),
                dma(SEND), dma(KC2),
                dma(SEND), dma(KC3),
                dma(2, SEND), dma(2, KC4),
                pltpu.SemaphoreType.REGULAR,
                dma(2, GSEND), dma(2, M1),
                dma(2, GSEND), dma(2, M2),
                dma(2, GSEND), dma(2, M3),
                dma(2, GSEND), dma(2, MO),
                dma(2, GSEND), dma(2, MI),
                dma(2, GSEND), dma(2, MP),
            ],
            compiler_params=pltpu.CompilerParams(
                collective_id=0, has_side_effects=True, vmem_limit_bytes=35 * 2**20
            ),
            name="mlp_all_reduce",
        )(x, w_gate, w_up, w_down)
        return pl.pallas_call(
            store_kernel,
            out_shape=jax.ShapeDtypeStruct((rows, D), BF16),
            in_specs=[any_spec],
            out_specs=any_spec,
            scratch_shapes=[dma(8)],
            compiler_params=pltpu.CompilerParams(vmem_limit_bytes=2**20),
            name="store",
        )(y)

    return jax.shard_map(
        step,
        mesh=mesh,
        in_specs=(P("dp", None), P(None, "tp"), P(None, "tp"), P("tp", None)),
        out_specs=P("dp", None),
        check_vma=False,
    )
```

```python
import functools

import jax
import jax.numpy as jnp
from jax import lax
from jax.experimental import pallas as pl
from jax.experimental.pallas import tpu as pltpu
from jax.sharding import PartitionSpec as P

MESH = pl.DeviceIdType.MESH
F32, BF16 = jnp.float32, jnp.bfloat16

ROWS_PER_CHUNK = 128
PIECES = 2
TAIL = 2
OFF = (0, 1, 3, 4, 5, 6, 7)
GOFF = (0, 2, 4, 6, 8, 10)
KP = 2 * (OFF[1] - OFF[0])
KX = 2 * (OFF[2] - OFF[1])
KZ1 = OFF[5] - OFF[2]
KZ2 = 2 * (OFF[4] - OFF[3])
KZ3 = OFF[5] - OFF[2]
KY = 2 * (OFF[6] - OFF[5])
KT = OFF[1] - OFF[0]
KO = OFF[5] - OFF[1]
KI = OFF[3] - OFF[1]
SEND = 3
PSEND = 2
KC1 = OFF[4] - OFF[1]
KC2 = 2 * (OFF[3] - OFF[2])
KC3 = OFF[5] - OFF[1]
KC4 = 2 * (OFF[5] - OFF[4])
KYS = max(SEND, OFF[6] - OFF[5] + 1)
M1 = GOFF[3] - GOFF[0]
M2 = 2 * (GOFF[2] - GOFF[1])
M3 = GOFF[3] - GOFF[0]
MO = 2 * GOFF[4] - GOFF[0] - GOFF[2]
MI = 2 * (GOFF[4] - GOFF[2])
MP = 2 * (GOFF[5] - GOFF[4])
GSEND = 6


def k_block(rows, F):
    return (rows - F) // 256 * 256


def split(W):
    return W * 6 // 7 // 128 * 128 if W > 256 else W // 2


def kernel(R, x_ref, wg_ref, wu_ref, wd_ref, y_ref, wrest, xbuf, hidden, term, acco, acci, pairsend, pairrecv,
           xsend, xrecv, z1send, z1recv, z2send, z2recv, z3send, z3recv, ysend, yrecv, fin,
           accco, accci, c1send, c1recv, c2send, c2recv, c3send, c3recv, c4send, c4recv,
           w_sem, x_sem, sp, rp, sx, rx, sz1, rz1, sz2, rz2, sz3, rz3, sy, ry,
           sc1, rc1, sc2, rc2, sc3, rc3, sc4, rc4, ready,
           sa1, ra1, sa2, ra2, sa3, ra3, sxo, rxo, sxi, rxi, spa, rpa):
    N = x_ref.shape[0] // R
    D = x_ref.shape[1]
    F = wg_ref.shape[1]
    W = D // 8
    W1 = split(W)
    Q = R // 2
    G = Q // PIECES
    NG = N * PIECES
    KB = k_block(y_ref.shape[0], F)
    NB = D // KB
    REST = D - NB * KB
    assert NB * 2 * F <= D

    me = lax.axis_index("tp")
    c = lax.rem(me, 2)
    z = lax.rem(me // 2, 4)
    yy = lax.rem(me // 8, 2)
    xx = me // 16
    odd = lax.rem(z, 2)
    s = z // 2
    is_end = lax.rem(z, 3) == 0
    is_mid = lax.rem(z, 3) != 0
    pair = me + 1 - 2 * c
    xp = me + 16 - 32 * xx
    yp = me + 8 - 16 * yy
    side = me + 2 - 4 * odd
    mid = jnp.where(is_mid, me + 6 - 4 * z, me)
    first = (xp, yp)
    last = (yp, xp)
    f = (xx, yy)

    out_rows = pl.multiple_of((1 - s) * Q, Q)
    in_rows = pl.multiple_of(s * Q, Q)

    def remote(src, dst, ss, rs, dev):
        return pltpu.make_async_remote_copy(
            src_ref=src, dst_ref=dst, send_sem=ss, recv_sem=rs, device_id={"tp": dev}, device_id_type=MESH
        )

    def weight_copies(b):
        copies = []
        for i, ref in enumerate((wg_ref, wu_ref)):
            if b < NB:
                dst = y_ref.at[pl.ds(F, KB), pl.ds((2 * b + i) * F, F)]
                src = ref.at[pl.ds(b * KB, KB)]
            else:
                dst = wrest.at[:, pl.ds(i * F, F)]
                src = ref.at[pl.ds(NB * KB, REST)]
            copies.append(pltpu.make_async_copy(src, dst, w_sem.at[b, i]))
        return copies

    down_copy = pltpu.make_async_copy(wd_ref, y_ref.at[pl.ds(0, F)], w_sem.at[NB + 1, 0])

    def x_copy(k):
        rows = pl.ds(pl.multiple_of(k * R, R), R)
        return pltpu.make_async_copy(x_ref.at[rows], xbuf.at[lax.rem(k, 2)], x_sem.at[lax.rem(k, 2)])

    x_copy(0).start()
    for b in range(NB + 1):
        for copy in weight_copies(b):
            copy.start()
    down_copy.start()

    barrier = pltpu.get_barrier_semaphore()
    for dev in (pair, xp, yp, side):
        pl.semaphore_signal(barrier, inc=1, device_id={"tp": dev}, device_id_type=MESH)

    @pl.when(is_mid)
    def _():
        pl.semaphore_signal(barrier, inc=1, device_id={"tp": mid}, device_id_type=MESH)
        pl.semaphore_wait(barrier, 5)

    @pl.when(is_end)
    def _():
        pl.semaphore_wait(barrier, 4)

    def c_pair(k):
        a, b = lax.rem(k, PSEND), lax.rem(k, KP)
        return remote(pairsend.at[a], pairrecv.at[b], sp.at[a], rp.at[b], pair)

    def c_first(k, t):
        a, b = lax.rem(k, SEND), lax.rem(k, KX)
        return remote(xsend.at[a, t], xrecv.at[b, t], sx.at[t, a], rx.at[t, b], first[t])

    def c_z1(k):
        a, b = lax.rem(k, SEND), lax.rem(k, KZ1)
        return remote(z1send.at[a], z1recv.at[b], sz1.at[a], rz1.at[b], side)

    def c_z2(k):
        a, b = lax.rem(k, SEND), lax.rem(k, KZ2)
        return remote(z2send.at[a], z2recv.at[b], sz2.at[a], rz2.at[b], mid)

    def c_z3(k):
        a, b = lax.rem(k, SEND), lax.rem(k, KZ3)
        return remote(z3send.at[a], z3recv.at[b], sz3.at[a], rz3.at[b], side)

    def c_last(k, t):
        a, b = lax.rem(k, KYS), lax.rem(k, KY)
        return remote(ysend.at[a, t], yrecv.at[b, t], sy.at[t, a], ry.at[t, b], last[t])

    def c_c1(k):
        a, b = lax.rem(k, SEND), lax.rem(k, KC1)
        return remote(c1send.at[a], c1recv.at[b], sc1.at[a], rc1.at[b], side)

    def c_c2(k):
        a, b = lax.rem(k, SEND), lax.rem(k, KC2)
        return remote(c2send.at[a], c2recv.at[b], sc2.at[a], rc2.at[b], mid)

    def c_c3(k):
        a, b = lax.rem(k, SEND), lax.rem(k, KC3)
        return remote(c3send.at[a], c3recv.at[b], sc3.at[a], rc3.at[b], side)

    def c_c4(k, t):
        a, b = lax.rem(k, SEND), lax.rem(k, KC4)
        return remote(c4send.at[a, t], c4recv.at[b, t], sc4.at[t, a], rc4.at[t, b], first[t])

    def block(t, flip=False):
        h = 1 - f[t] if flip else f[t]
        return pl.ds(pl.multiple_of((c * 4 + t * 2 + h) * W, 128), W)

    def y_piece(p, at, t):
        row = (p // PIECES) * R + at + lax.rem(p, PIECES) * G
        return y_ref.at[pl.ds(pl.multiple_of(row, G), G), block(t)]

    def fin_piece(p, t):
        return fin.at[p // PIECES, t, pl.ds(pl.multiple_of(lax.rem(p, PIECES) * G, G), G)]

    def c_a1(p, t):
        a, b = lax.rem(p, GSEND), lax.rem(p, M1)
        return remote(fin_piece(p, t), y_piece(p, out_rows, t), sa1.at[t, a], ra1.at[t, b], side)

    def c_a2(p, t):
        a, b = lax.rem(p, GSEND), lax.rem(p, M2)
        piece = y_piece(p, out_rows, t)
        return remote(piece, piece, sa2.at[t, a], ra2.at[t, b], mid)

    def c_a3(p, t):
        a, b = lax.rem(p, GSEND), lax.rem(p, M3)
        piece = y_piece(p, in_rows, t)
        return remote(piece, piece, sa3.at[t, a], ra3.at[t, b], side)

    def c_xo(p, t, src=None):
        a, b = lax.rem(p, GSEND), lax.rem(p, MO)
        piece = y_piece(p, out_rows, t)
        return remote(piece if src is None else src, piece, sxo.at[t, a], rxo.at[t, b], first[t])

    def c_xi(p, t):
        a, b = lax.rem(p, GSEND), lax.rem(p, MI)
        piece = y_piece(p, in_rows, t)
        return remote(piece, piece, sxi.at[t, a], rxi.at[t, b], first[t])

    def c_pa(p, h):
        a, b = lax.rem(p, GSEND), lax.rem(p, MP)
        row = (p // PIECES) * R + h * Q + lax.rem(p, PIECES) * G
        piece = y_ref.at[pl.ds(pl.multiple_of(row, G), G), pl.ds(pl.multiple_of(c * 4 * W, 128), 4 * W)]
        return remote(piece, piece, spa.at[h, a], rpa.at[h, b], pair)

    def h0(k):
        @pl.when(k + 1 < N)
        def _():
            x_copy(k + 1).start()

        x_copy(k).wait()
        xs = lax.rem(k, 2)
        h = None
        for b in range(NB + 1):
            @pl.when(k == 0)
            def _():
                for copy in weight_copies(b):
                    copy.wait()

            rows = y_ref[F:F + KB, b * 2 * F:(b + 1) * 2 * F] if b < NB else wrest[...]
            part = jnp.dot(xbuf[xs, :, b * KB:min(D, (b + 1) * KB)], rows, preferred_element_type=F32)
            h = part if h is None else h + part
        hidden[...] = (jax.nn.silu(h[:, :F]) * h[:, F:]).astype(BF16)

    def s0(k):
        @pl.when(k == 0)
        def _():
            down_copy.wait()

        for t in range(2):
            cols = pl.ds(pl.multiple_of((1 - c) * 4 * W + t * 2 * W, 128), 2 * W)
            part = jnp.dot(hidden[...], y_ref[:F, cols], preferred_element_type=F32)
            for i in range(2):
                pairsend[lax.rem(k, PSEND), t, i] = part[:, i * W:(i + 1) * W].astype(BF16)
        c_pair(k).start()
        for t in range(2):
            cols = pl.ds(pl.multiple_of(c * 4 * W + t * 2 * W, 128), 2 * W)
            part = jnp.dot(hidden[...], y_ref[:F, cols], preferred_element_type=F32)
            for i in range(2):
                term[lax.rem(k, KT), t, i] = part[:, i * W:(i + 1) * W]

        @pl.when(k == N - 1)
        def _():
            for dev in (pair, xp, yp, side):
                pl.semaphore_signal(ready, inc=1, device_id={"tp": dev}, device_id_type=MESH)

            @pl.when(is_mid)
            def _():
                pl.semaphore_signal(ready, inc=1, device_id={"tp": mid}, device_id_type=MESH)

    def s1(k):
        c_pair(k).wait_recv()
        a, b, kt = lax.rem(k, SEND), lax.rem(k, KP), lax.rem(k, KT)
        ki, ko = lax.rem(k, KI), lax.rem(k, KO)
        for t in range(2):
            h = 1 - f[t]
            xsend[a, t] = (term[kt, t, h, :, :W1] + pairrecv[b, t, h, :, :W1].astype(F32)).astype(BF16)
            c_first(k, t).start()
        for t in range(2):
            for h in range(2):
                for dst, slot, at in ((accci, ki, in_rows), (accco, ko, out_rows)):
                    rows = pl.ds(at, Q)
                    dst[slot, t, h] = term[kt, t, h, rows, W1:] + pairrecv[b, t, h, rows, W1:].astype(F32)

        @pl.when(is_end)
        def _():
            c1send[a] = accci[ki].astype(BF16)
            c_c1(k).start()

        for t in range(2):
            h = f[t]
            for dst, slot, at in ((acci, ki, in_rows), (acco, ko, out_rows)):
                rows = pl.ds(at, Q)
                dst[slot, t] = term[kt, t, h, rows, :W1] + pairrecv[b, t, h, rows, :W1].astype(F32)

    def s2(k):
        a, b, ki, ko = lax.rem(k, SEND), lax.rem(k, KX), lax.rem(k, KI), lax.rem(k, KO)

        @pl.when(is_mid)
        def _():
            c_c1(k).wait_recv()
            c2send[a] = (accci[ki] + c1recv[lax.rem(k, KC1)].astype(F32)).astype(BF16)
            c_c2(k).start()

        for t in range(2):
            c_first(k, t).wait_recv()
            acci[ki, t] = acci[ki, t] + xrecv[b, t, pl.ds(in_rows, Q)].astype(F32)
            acco[ko, t] = acco[ko, t] + xrecv[b, t, pl.ds(out_rows, Q)].astype(F32)

        @pl.when(is_end)
        def _():
            z1send[a] = acci[ki].astype(BF16)
            c_z1(k).start()

    def s3(k):
        @pl.when(is_mid)
        def _():
            a, b, ki, ko = lax.rem(k, SEND), lax.rem(k, KZ1), lax.rem(k, KI), lax.rem(k, KO)
            c_c2(k).wait_recv()
            c3send[a] = (accco[ko] + c2recv[lax.rem(k, KC2)].astype(F32)).astype(BF16)
            c_c3(k).start()
            c_z1(k).wait_recv()
            z2send[a] = (acci[ki] + z1recv[b].astype(F32)).astype(BF16)
            c_z2(k).start()

    def s4(k):
        a, b, ko = lax.rem(k, SEND), lax.rem(k, KZ2), lax.rem(k, KO)

        @pl.when(is_end)
        def _():
            c_c3(k).wait_recv()
            for t in range(2):
                h = 1 - f[t]
                c4send[a, t] = (accco[ko, t, h] + c3recv[lax.rem(k, KC3), t, h].astype(F32)).astype(BF16)
                c_c4(k, t).start()

        @pl.when(is_mid)
        def _():
            c_z2(k).wait_recv()
            z3send[a] = (acco[ko] + z2recv[b].astype(F32)).astype(BF16)
            c_z3(k).start()

    def s5(k):
        @pl.when(is_end)
        def _():
            a, b, ko = lax.rem(k, KYS), lax.rem(k, KZ3), lax.rem(k, KO)
            for t in range(2):
                h = f[t]
                c_c4(k, t).wait_recv()
                ysend[a, t, :, W1:] = (
                    accco[ko, t, h]
                    + c3recv[lax.rem(k, KC3), t, h].astype(F32)
                    + c4recv[lax.rem(k, KC4), t].astype(F32)
                ).astype(BF16)
            c_z3(k).wait_recv()
            for t in range(2):
                ysend[a, t, :, :W1] = (acco[ko, t] + z3recv[b, t].astype(F32)).astype(BF16)
                c_last(k, t).start()

    def s6(k):
        @pl.when(is_end)
        def _():
            a, b = lax.rem(k, KYS), lax.rem(k, KY)
            for t in range(2):
                c_last(k, t).wait_recv()
                fin[k, t] = (ysend[a, t].astype(F32) + yrecv[b, t].astype(F32)).astype(BF16)

    def open_gather():
        @pl.when(is_mid)
        def _():
            pl.semaphore_wait(ready, 5)

        @pl.when(is_end)
        def _():
            pl.semaphore_wait(ready, 4)

    def g0(p):
        @pl.when(is_end)
        def _():
            for t in range(2):
                c_a1(p, t).start()
                c_xo(p, t, fin_piece(p, t)).start()
            for t in range(2):
                y_piece(p, out_rows, t)[...] = fin_piece(p, t)[...]

    def g1(p):
        @pl.when(is_mid)
        def _():
            for t in range(2):
                c_a1(p, t).wait_recv()
                c_a2(p, t).start()
                c_xo(p, t).start()

    def g2(p):
        @pl.when(is_mid)
        def _():
            for t in range(2):
                c_a2(p, t).wait_recv()
                c_a3(p, t).start()
                c_xi(p, t).start()

    def g3(p):
        @pl.when(is_end)
        def _():
            for t in range(2):
                c_a3(p, t).wait_recv()
                c_xi(p, t).start()

    def g4(p):
        for t in range(2):
            c_xo(p, t).wait_recv()
            c_xi(p, t).wait_recv()
        for h in range(2):
            c_pa(p, h).start()

    def g5(p):
        for h in range(2):
            c_pa(p, h).wait_recv()

    def d0(k):
        c_pair(k).wait_send()

    def d1(k):
        for t in range(2):
            c_first(k, t).wait_send()

        @pl.when(is_end)
        def _():
            c_c1(k).wait_send()

    def d2(k):
        @pl.when(is_end)
        def _():
            c_z1(k).wait_send()

        @pl.when(is_mid)
        def _():
            c_c2(k).wait_send()

    def d3(k):
        @pl.when(is_mid)
        def _():
            c_c3(k).wait_send()
            c_z2(k).wait_send()

    def d4(k):
        @pl.when(is_end)
        def _():
            for t in range(2):
                c_c4(k, t).wait_send()

        @pl.when(is_mid)
        def _():
            c_z3(k).wait_send()

    def d5(k):
        @pl.when(is_end)
        def _():
            for t in range(2):
                c_last(k, t).wait_send()

    def e0(p):
        @pl.when(is_end)
        def _():
            for t in range(2):
                c_a1(p, t).wait_send()
                c_xo(p, t, fin_piece(p, t)).wait_send()

    def e1(p):
        @pl.when(is_mid)
        def _():
            for t in range(2):
                c_a2(p, t).wait_send()
                c_xo(p, t).wait_send()

    def e2(p):
        @pl.when(is_mid)
        def _():
            for t in range(2):
                c_a3(p, t).wait_send()
                c_xi(p, t).wait_send()

    def e3(p):
        @pl.when(is_end)
        def _():
            for t in range(2):
                c_xi(p, t).wait_send()

    def e4(p):
        for h in range(2):
            c_pa(p, h).wait_send()

    reduce_stages = (
        (s0, d0, PSEND), (s1, d1, SEND), (h0, None, 0), (s2, d2, SEND), (s3, d3, SEND), (s4, d4, SEND), (s5, d5, KYS),
        (s6, None, 0),
    )
    gather_stages = (
        (g0, e0, GSEND), (g1, e1, GSEND), (g2, e2, GSEND), (g3, e3, GSEND), (g4, e4, GSEND), (g5, None, 0),
    )

    def advance(i, count, offsets, stages):
        for off, (run, drain, lag) in reversed(tuple(zip(offsets, stages))):
            if drain is not None:
                k_old = i - off - lag

                @pl.when((k_old >= 0) & (k_old < count))
                def _():
                    drain(k_old)

            if run is not None:
                k = i - off

                @pl.when((k >= 0) & (k < count))
                def _():
                    run(k)

    offsets = OFF[:2] + OFF[:1] + OFF[2:]
    tail_stages = ((None, d0, PSEND), reduce_stages[1], (None, None, 0)) + reduce_stages[3:]

    def reduce_tick(i, carry):
        advance(i, N, offsets, reduce_stages)
        return carry

    def gather_tick(u, carry):
        @pl.when(lax.rem(u, TAIL) == 0)
        def _():
            advance(N + u // TAIL, N, offsets, tail_stages)

        advance(u, NG, GOFF, gather_stages)
        return carry

    lax.fori_loop(0, N, reduce_tick, 0)
    open_gather()
    ticks = NG + max(off + lag for off, (_, _, lag) in zip(GOFF, gather_stages))
    lax.fori_loop(0, ticks, gather_tick, 0)


def store_kernel(y_ref, o_ref, sem):
    blocks = sem.shape[0]
    rows = y_ref.shape[0] // blocks
    copies = [
        pltpu.make_async_copy(y_ref.at[pl.ds(i * rows, rows)], o_ref.at[pl.ds(i * rows, rows)], sem.at[i])
        for i in range(blocks)
    ]
    for copy in copies:
        copy.start()
    for copy in copies:
        copy.wait()


def solution(mesh):
    def step(x, w_gate, w_up, w_down):
        rows, D = x.shape
        F = w_gate.shape[1]
        R = min(ROWS_PER_CHUNK, rows // 8)
        W, Q = D // 8, R // 2
        W1 = split(W)
        W3 = W - W1
        any_spec = pl.BlockSpec(memory_space=pl.ANY)
        dma = lambda *shape: pltpu.SemaphoreType.DMA(shape)
        kb = k_block(rows, F)
        blocks = D // kb + 2
        y = pl.pallas_call(
            functools.partial(kernel, R),
            out_shape=pltpu.VMEM((rows, D), BF16),
            in_specs=[any_spec] * 4,
            out_specs=pl.BlockSpec(memory_space=pltpu.VMEM),
            scratch_shapes=[
                pltpu.VMEM((D % kb, 2 * F), BF16),
                pltpu.VMEM((2, R, D), BF16),
                pltpu.VMEM((R, F), BF16),
                pltpu.VMEM((KT, 2, 2, R, W), F32),
                pltpu.VMEM((KO, 2, Q, W1), F32),
                pltpu.VMEM((KI, 2, Q, W1), F32),
                pltpu.VMEM((PSEND, 2, 2, R, W), BF16),
                pltpu.VMEM((KP, 2, 2, R, W), BF16),
                pltpu.VMEM((SEND, 2, R, W1), BF16),
                pltpu.VMEM((KX, 2, R, W1), BF16),
                pltpu.VMEM((SEND, 2, Q, W1), BF16),
                pltpu.VMEM((KZ1, 2, Q, W1), BF16),
                pltpu.VMEM((SEND, 2, Q, W1), BF16),
                pltpu.VMEM((KZ2, 2, Q, W1), BF16),
                pltpu.VMEM((SEND, 2, Q, W1), BF16),
                pltpu.VMEM((KZ3, 2, Q, W1), BF16),
                pltpu.VMEM((KYS, 2, Q, W), BF16),
                pltpu.VMEM((KY, 2, Q, W), BF16),
                pltpu.VMEM((rows // R, 2, Q, W), BF16),
                pltpu.VMEM((KO, 2, 2, Q, W3), F32),
                pltpu.VMEM((KI, 2, 2, Q, W3), F32),
                pltpu.VMEM((SEND, 2, 2, Q, W3), BF16),
                pltpu.VMEM((KC1, 2, 2, Q, W3), BF16),
                pltpu.VMEM((SEND, 2, 2, Q, W3), BF16),
                pltpu.VMEM((KC2, 2, 2, Q, W3), BF16),
                pltpu.VMEM((SEND, 2, 2, Q, W3), BF16),
                pltpu.VMEM((KC3, 2, 2, Q, W3), BF16),
                pltpu.VMEM((SEND, 2, Q, W3), BF16),
                pltpu.VMEM((KC4, 2, Q, W3), BF16),
                dma(blocks, 2), dma(2),
                dma(PSEND), dma(KP),
                dma(2, SEND), dma(2, KX),
                dma(SEND), dma(KZ1),
                dma(SEND), dma(KZ2),
                dma(SEND), dma(KZ3),
                dma(2, KYS), dma(2, KY),
                dma(SEND), dma(KC1),
                dma(SEND), dma(KC2),
                dma(SEND), dma(KC3),
                dma(2, SEND), dma(2, KC4),
                pltpu.SemaphoreType.REGULAR,
                dma(2, GSEND), dma(2, M1),
                dma(2, GSEND), dma(2, M2),
                dma(2, GSEND), dma(2, M3),
                dma(2, GSEND), dma(2, MO),
                dma(2, GSEND), dma(2, MI),
                dma(2, GSEND), dma(2, MP),
            ],
            compiler_params=pltpu.CompilerParams(
                collective_id=0, has_side_effects=True, vmem_limit_bytes=35 * 2**20
            ),
            name="mlp_all_reduce",
        )(x, w_gate, w_up, w_down)
        return pl.pallas_call(
            store_kernel,
            out_shape=jax.ShapeDtypeStruct((rows, D), BF16),
            in_specs=[any_spec],
            out_specs=any_spec,
            scratch_shapes=[dma(8)],
            compiler_params=pltpu.CompilerParams(vmem_limit_bytes=2**20),
            name="store",
        )(y)

    return jax.shard_map(
        step,
        mesh=mesh,
        in_specs=(P("dp", None), P(None, "tp"), P(None, "tp"), P("tp", None)),
        out_specs=P("dp", None),
        check_vma=False,
    )
```
